32 devices in a mesh: seq: 8 (over z, x), hid: 4 (over y, core).
Axes of the slice: x: 2, y: 2, z: 4, core: 2. Of those that a mesh axis runs over, the one named last changes fastest.
Arguments:
- hidden: bfloat16 [8192, 4096], P('seq', 'hid'), may hold values from -40 to 40, as said below
- seg_ids: int32 [8192], P('seq'), may hold values from 0 to 31, as said below
- lengths: int32 [32], replicated, may hold values from 64 to 4096, as said below
- owner_slot: int32 [32], replicated, may hold values from 0 to 31, each once
- pool_bias: float32 [4096], P('hid'), may hold values from -3 to 3
Outputs:
- pooled: bfloat16 [32, 4096], P('seq', 'hid')
The draws below stay inside these ranges and needn't reach their ends.
Inputs may be any that keep to these rules, and one draw needn't show every extreme that they name: `hidden`: float values; each feature's scale differs. `seg_ids`: never falls along the stream; document d occupies exactly lengths[d] consecutive tokens, documents in order. `lengths`: they sum to 8192; one of them is exactly 4096; the first 16 documents each have 1024 // 16 tokens and so fill the first index's tokens; hence at most 16 documents end within one index's tokens, and the first index has exactly 16. `owner_slot`: each row number once.
All inputs are finite; a program needn't handle non-finite values.
Results may differ from the reference program's by a relative error of at most 0.001.
Values may be sent and summed in bfloat16 or wider, within the bound.
A program may use at most 64 MiB of HBM per device.

```python
import math
import jax
import jax.numpy as jnp
from jax import lax

D = 4096
TOK_DEV = 1024
FIN = 16
TOKENS = 8192
DOCS = 32
MOST = 4096
N_SEQ = 8


def doc_lengths(key):
    floor_size = TOK_DEV // FIN
    remaining = TOKENS - MOST - TOK_DEV
    others = DOCS - 1 - FIN
    even_share = remaining // others
    leftover = remaining % others
    positions = jnp.arange(others, dtype=jnp.int32)
    doc_sizes = even_share + (positions < leftover).astype(jnp.int32)
    pair_count = others // 2
    for sweep_index in range(6):
        key, pair_key, move_key = jax.random.split(key, 3)
        shuffled = jax.random.permutation(pair_key, others).astype(jnp.int32)
        giver = shuffled[0:2 * pair_count:2]
        taker = shuffled[1:2 * pair_count:2]
        headroom = jnp.minimum(doc_sizes[giver] - floor_size, MOST - doc_sizes[taker])
        transfer = jax.random.randint(move_key, (pair_count,), 0, headroom + 1).astype(jnp.int32)
        doc_sizes = doc_sizes.at[giver].add(-transfer).at[taker].add(transfer)
    tail_count = others + 1
    long_index = jax.random.randint(key, (), 0, tail_count).astype(jnp.int32)
    tail_iota = jnp.arange(tail_count, dtype=jnp.int32)
    shifted = jnp.clip(jnp.where(tail_iota < long_index, tail_iota, tail_iota - 1), 0, others - 1)
    tail = jnp.where(tail_iota == long_index, MOST, doc_sizes[shifted])
    head = jnp.full((FIN,), floor_size, jnp.int32)
    return jnp.concatenate([head, tail.astype(jnp.int32)]).astype(jnp.int32)


def draw_lengths(key, part):
    return doc_lengths(jax.random.fold_in(key, 11))


def draw_seg_ids(key, part):
    sizes_drawn = doc_lengths(jax.random.fold_in(key, 11))
    starts = jnp.cumsum(sizes_drawn) - sizes_drawn
    marks = jnp.zeros((TOKENS,), jnp.int32).at[starts[1:]].add(1)
    return jnp.cumsum(marks).astype(jnp.int32)


def draw_hidden(key, part):
    col_key = jax.random.fold_in(key, 0)
    value_key = jax.random.fold_in(key, 2)
    rising = jnp.exp2(jnp.arange(D, dtype=jnp.float32) / D)
    columns = jnp.exp(jax.random.uniform(col_key, (D,), jnp.float32, math.log(0.7), math.log(1.4)))
    values = jnp.clip(jax.random.normal(value_key, (TOKENS, D), jnp.float32), -4.0, 4.0)
    result = values * (columns * rising)[None, :]
    return result.astype(jnp.bfloat16)


def shard_levels(own_key, shape, cuts, least, high):
    def one(axis_at, shards_of):
        steps = jax.random.uniform(jax.random.fold_in(jax.random.fold_in(own_key, 6), axis_at), (shards_of,), jnp.float32, least / len(cuts), high / len(cuts))
        return jnp.repeat(jnp.exp(steps), shape[axis_at] // shards_of).reshape((-1,) + (1,) * (len(shape) - axis_at - 1))

    loudness = one(*cuts[0])
    for cut in cuts[1:]:
        loudness = loudness * one(*cut)
    return loudness


def centred(own_key, dims, scale, limit, pieces=(), kind=jnp.bfloat16):
    values = jax.random.normal(own_key, dims, jnp.float32) * scale
    if len(pieces) > 0:
        values = shard_levels(own_key, dims, pieces, -0.22, 0.18) * values
    return jnp.clip(values, min=-limit, max=limit).astype(kind)


def setup_inputs(seed: int = 0) -> dict:
    key_list = jax.random.split(jax.random.key(seed), 6)
    hidden = draw_hidden(jax.random.fold_in(key_list[5], 71), 0)
    seg_ids = draw_seg_ids(jax.random.fold_in(key_list[5], 71), 0)
    lengths = draw_lengths(jax.random.fold_in(key_list[5], 71), 0)
    owner_slot = jax.random.permutation(key_list[3], DOCS).astype(jnp.int32)
    pool_bias = centred(key_list[4], (D,), 0.5, 3.0, ((0, 4),), jnp.float32)
    return {"hidden": hidden, "seg_ids": seg_ids, "lengths": lengths, "owner_slot": owner_slot, "pool_bias": pool_bias}


def reference(hidden, seg_ids, lengths, owner_slot, pool_bias):
    token_blocks = hidden.reshape(N_SEQ, TOK_DEV, D)
    block_ids = seg_ids.reshape(N_SEQ, TOK_DEV)

    def accumulate(running, operands):
        token_block, block_docs = operands
        added = jax.ops.segment_sum(token_block.astype(jnp.float32), block_docs, num_segments=DOCS)
        return (running + added, None)
    totals, _ = lax.scan(accumulate, jnp.zeros((DOCS, D), jnp.float32), (token_blocks, block_ids))
    averages = totals / lengths.astype(jnp.float32)[:, None] + pool_bias[None, :]
    energy = lax.optimization_barrier(jnp.mean(averages * averages, axis=1, keepdims=True))
    normed = averages * lax.rsqrt(energy + 1e-06)
    placed = jnp.zeros((DOCS, D), jnp.float32).at[owner_slot].set(normed)
    return placed.astype(jnp.bfloat16)
```

```python
import functools

import jax
import jax.numpy as jnp
from jax import lax
from jax.experimental import pallas as pl
from jax.experimental.pallas import tpu as pltpu
from jax.sharding import PartitionSpec as P

MESH = pl.DeviceIdType.MESH
LANES = 128


def kernel(
    n_seq, n_hid, chunks, pad,
    hidden_hbm, seg_hbm, len_hbm, slot_hbm, bias_hbm,
    out_ref,
    hidden, seg, lens, slots, bias, parts, landed, mine, squares, squares_in,
    load_sems, small_sems, send_sems, recv_sems, sq_send_sems, sq_recv_sems,
):
    me = lax.axis_index("seq")
    my_hid = lax.axis_index("hid")
    tokens, width = hidden.shape
    docs = lens.shape[1]
    per_owner = docs // n_seq
    step = width // chunks
    features = width * n_hid

    def loader(c):
        cols = pl.ds(c * step, step)
        return pltpu.make_async_copy(hidden_hbm.at[:, cols], hidden.at[:, cols], load_sems.at[c])

    small = [
        pltpu.make_async_copy(src, dst, small_sems.at[i])
        for i, (src, dst) in enumerate(
            ((slot_hbm, slots), (seg_hbm, seg), (len_hbm, lens), (bias_hbm, bias))
        )
    ]
    small[0].start()
    small[1].start()
    loads = [loader(c) for c in range(chunks)]
    for load in loads:
        load.start()
    small[2].start()
    small[3].start()

    barrier = pltpu.get_barrier_semaphore()
    for k in range(1, n_seq):
        pl.semaphore_signal(
            barrier, inc=1, device_id={"seq": lax.rem(me + k, n_seq)}, device_id_type=MESH
        )
    for k in range(1, n_hid):
        pl.semaphore_signal(
            barrier, inc=1, device_id={"hid": lax.rem(my_hid + k, n_hid)}, device_id_type=MESH
        )

    small[0].wait()
    row = lax.broadcasted_iota(jnp.int32, (n_seq * pad, 1), 0)
    inner = row % pad
    row_slot = jnp.where(inner < per_owner, (row // pad) * per_owner + inner, -1)
    doc_iota = lax.broadcasted_iota(jnp.int32, (1, docs), 1).astype(jnp.float32)
    found = jnp.where(row_slot == slots[...], doc_iota + 1.0, 0.0)
    row_doc = jnp.sum(found, axis=1, keepdims=True).astype(jnp.int32) - 1
    small[1].wait()
    picker = jnp.concatenate(
        [
            jnp.where(row_doc == seg[k : k + 1, :], 1.0, 0.0).astype(jnp.bfloat16)
            for k in range(tokens // LANES)
        ],
        axis=1,
    )

    def sender(c, k):
        cols = pl.ds(c * step, step)
        peer = lax.rem(me + k, n_seq)
        return pltpu.make_async_remote_copy(
            src_ref=parts.at[peer, :, cols],
            dst_ref=landed.at[k - 1, :, cols],
            send_sem=send_sems.at[c, k - 1],
            recv_sem=recv_sems.at[c, k - 1],
            device_id={"seq": peer},
            device_id_type=MESH,
        )

    order = sorted(range(1, n_seq), key=lambda k: -min(k, n_seq - k))
    for c in range(chunks):
        cols = pl.ds(c * step, step)
        loads[c].wait()
        product = jnp.dot(picker, hidden[:, cols], preferred_element_type=jnp.float32)
        for p in range(n_seq):
            parts[p, :, cols] = product[p * pad : p * pad + per_owner, :]
        if c == 0:
            pl.semaphore_wait(barrier, n_seq - 1 + n_hid - 1)
        for k in order:
            sender(c, k).start()

    small[2].wait()
    small[3].wait()
    wanted = lax.broadcasted_iota(jnp.int32, (per_owner, 1), 0) + me * per_owner
    my_len = jnp.sum(
        jnp.where(wanted == slots[...], lens[...].astype(jnp.float32), 0.0), axis=1, keepdims=True
    )

    lane_sq = jnp.zeros((per_owner, LANES), jnp.float32)
    for c in range(chunks):
        cols = pl.ds(c * step, step)
        total = parts[me, :, cols]
        for k in order[::-1]:
            sender(c, k).wait_recv()
            total = total + landed[k - 1, :, cols]
        averages = total / my_len + bias[:, cols]
        mine[:, cols] = averages
        for j in range(step // LANES):
            piece = averages[:, j * LANES : (j + 1) * LANES]
            lane_sq = lane_sq + piece * piece
    squares[...] = lane_sq

    sq_copies = []
    for k in range(1, n_hid):
        copy = pltpu.make_async_remote_copy(
            src_ref=squares,
            dst_ref=squares_in.at[k - 1],
            send_sem=sq_send_sems.at[k - 1],
            recv_sem=sq_recv_sems.at[k - 1],
            device_id={"hid": lax.rem(my_hid + k, n_hid)},
            device_id_type=MESH,
        )
        copy.start()
        sq_copies.append(copy)
    for c in range(chunks):
        for k in order:
            sender(c, k).wait_send()
    for k in range(1, n_hid):
        sq_copies[k - 1].wait_recv()
        lane_sq = lane_sq + squares_in[k - 1]
    energy = jnp.sum(lane_sq, axis=1, keepdims=True) / features
    out_ref[...] = (mine[...] * lax.rsqrt(energy + 1e-06)).astype(jnp.bfloat16)
    for copy in sq_copies:
        copy.wait_send()


def local(n_seq, n_hid, hidden, seg_ids, lengths, owner_slot, pool_bias):
    tokens, width = hidden.shape
    docs = lengths.shape[0]
    per_owner = docs // n_seq
    pad = -(-per_owner // 8) * 8
    chunks = 4
    f32 = jnp.float32
    dma = pltpu.SemaphoreType.DMA
    return pl.pallas_call(
        functools.partial(kernel, n_seq, n_hid, chunks, pad),
        out_shape=jax.ShapeDtypeStruct((per_owner, width), jnp.bfloat16),
        in_specs=[pl.BlockSpec(memory_space=pl.ANY)] * 5,
        out_specs=pl.BlockSpec(memory_space=pltpu.VMEM),
        scratch_shapes=[
            pltpu.VMEM((tokens, width), jnp.bfloat16),
            pltpu.VMEM((tokens // LANES, LANES), jnp.int32),
            pltpu.VMEM((1, docs), jnp.int32),
            pltpu.VMEM((1, docs), jnp.int32),
            pltpu.VMEM((1, width), f32),
            pltpu.VMEM((n_seq, per_owner, width), f32),
            pltpu.VMEM((n_seq - 1, per_owner, width), f32),
            pltpu.VMEM((per_owner, width), f32),
            pltpu.VMEM((per_owner, LANES), f32),
            pltpu.VMEM((n_hid - 1, per_owner, LANES), f32),
            dma((chunks,)),
            dma((4,)),
            dma((chunks, n_seq - 1)),
            dma((chunks, n_seq - 1)),
            dma((n_hid - 1,)),
            dma((n_hid - 1,)),
        ],
        compiler_params=pltpu.CompilerParams(collective_id=0, has_side_effects=True),
    )(
        hidden,
        seg_ids.reshape(tokens // LANES, LANES),
        lengths.reshape(1, docs),
        owner_slot.reshape(1, docs),
        pool_bias.reshape(1, width),
    )


def solution(mesh):
    placed = (P("seq", "hid"), P("seq"), P(), P(), P("hid"))
    return jax.shard_map(
        functools.partial(local, mesh.shape["seq"], mesh.shape["hid"]),
        mesh=mesh,
        in_specs=placed,
        out_specs=P("seq", "hid"),
        check_vma=False,
    )
```

```python
import functools

import jax
import jax.numpy as jnp
from jax import lax
from jax.experimental import pallas as pl
from jax.experimental.pallas import tpu as pltpu
from jax.sharding import PartitionSpec as P

MESH = pl.DeviceIdType.MESH
LANES = 128


def kernel(
    n_seq, n_hid, chunks, pad,
    hidden_hbm, seg_hbm, len_hbm, slot_hbm, bias_hbm,
    out_ref,
    hidden, seg, lens, slots, bias, parts, landed, squares, squares_in,
    load_sems, small_sems, send_sem, recv_sem, sq_send_sem, sq_recv_sem,
):
    me = lax.axis_index("seq")
    my_hid = lax.axis_index("hid")
    tokens, width = hidden.shape
    docs = lens.shape[1]
    per_owner = docs // n_seq
    step = width // chunks
    features = width * n_hid
    order = sorted(range(1, n_seq), key=lambda k: -min(k, n_seq - k))
    peers = {k: lax.rem(me + k, n_seq) for k in order}
    hid_peers = {k: lax.rem(my_hid + k, n_hid) for k in range(1, n_hid)}

    barrier = pltpu.get_barrier_semaphore()
    for k in order:
        pl.semaphore_signal(barrier, inc=1, device_id={"seq": peers[k]}, device_id_type=MESH)
    for k in range(1, n_hid):
        pl.semaphore_signal(barrier, inc=1, device_id={"hid": hid_peers[k]}, device_id_type=MESH)

    def loader(c):
        cols = pl.ds(c * step, step)
        return pltpu.make_async_copy(hidden_hbm.at[:, cols], hidden.at[:, cols], load_sems.at[c])

    small = [
        pltpu.make_async_copy(src, dst, small_sems.at[i])
        for i, (src, dst) in enumerate(
            ((slot_hbm, slots), (seg_hbm, seg), (len_hbm, lens), (bias_hbm, bias))
        )
    ]
    small[0].start()
    small[1].start()
    loads = [loader(c) for c in range(chunks)]
    for load in loads:
        load.start()
    small[2].start()
    small[3].start()

    small[0].wait()
    row = lax.broadcasted_iota(jnp.int32, (n_seq * pad, 1), 0)
    inner = row % pad
    row_slot = jnp.where(inner < per_owner, (row // pad) * per_owner + inner, -1)
    doc_iota = lax.broadcasted_iota(jnp.int32, (1, docs), 1).astype(jnp.float32)
    found = jnp.where(row_slot == slots[...], doc_iota + 1.0, 0.0)
    row_doc = jnp.sum(found, axis=1, keepdims=True).astype(jnp.int32) - 1
    small[1].wait()
    picker = jnp.concatenate(
        [
            jnp.where(row_doc == seg[k : k + 1, :], 1.0, 0.0).astype(jnp.bfloat16)
            for k in range(tokens // LANES)
        ],
        axis=1,
    )

    def sender(c, k):
        cols = pl.ds(c * step, step)
        peer = peers[k]
        return pltpu.make_async_remote_copy(
            src_ref=parts.at[peer, :, cols],
            dst_ref=landed.at[k - 1, :, cols],
            send_sem=send_sem,
            recv_sem=recv_sem,
            device_id={"seq": peer},
            device_id_type=MESH,
        )

    for c in range(chunks):
        cols = pl.ds(c * step, step)
        loads[c].wait()
        product = jnp.dot(picker, hidden[:, cols], preferred_element_type=jnp.float32)
        for p in range(n_seq):
            parts[p, :, cols] = product[p * pad : p * pad + per_owner, :]
        if c == 0:
            pl.semaphore_wait(barrier, n_seq - 1 + n_hid - 1)
        for k in order:
            sender(c, k).start()

    small[2].wait()
    small[3].wait()
    wanted = lax.broadcasted_iota(jnp.int32, (per_owner, 1), 0) + me * per_owner
    my_len = jnp.sum(
        jnp.where(wanted == slots[...], lens[...].astype(jnp.float32), 0.0), axis=1, keepdims=True
    )

    pltpu.make_async_copy(landed, landed, recv_sem).wait()
    total = parts[me]
    for k in range(n_seq - 1):
        total = total + landed[k]
    averages = total / my_len + bias[...]
    lane_sq = jnp.zeros((per_owner, LANES), jnp.float32)
    for j in range(width // LANES):
        piece = averages[:, j * LANES : (j + 1) * LANES]
        lane_sq = lane_sq + piece * piece
    squares[...] = lane_sq

    for k in range(1, n_hid):
        pltpu.make_async_remote_copy(
            src_ref=squares,
            dst_ref=squares_in.at[k - 1],
            send_sem=sq_send_sem,
            recv_sem=sq_recv_sem,
            device_id={"hid": hid_peers[k]},
            device_id_type=MESH,
        ).start()
    pltpu.make_async_copy(landed, landed, send_sem).wait()
    pltpu.make_async_copy(squares_in, squares_in, sq_recv_sem).wait()
    for k in range(n_hid - 1):
        lane_sq = lane_sq + squares_in[k]
    energy = jnp.sum(lane_sq, axis=1, keepdims=True) / features
    out_ref[...] = (averages * lax.rsqrt(energy + 1e-06)).astype(jnp.bfloat16)
    pltpu.make_async_copy(squares_in, squares_in, sq_send_sem).wait()


def local(n_seq, n_hid, hidden, seg_ids, lengths, owner_slot, pool_bias):
    tokens, width = hidden.shape
    docs = lengths.shape[0]
    per_owner = docs // n_seq
    pad = -(-per_owner // 8) * 8
    chunks = 4
    f32 = jnp.float32
    dma = pltpu.SemaphoreType.DMA
    return pl.pallas_call(
        functools.partial(kernel, n_seq, n_hid, chunks, pad),
        out_shape=pltpu.VMEM((per_owner, width), jnp.bfloat16),
        in_specs=[pl.BlockSpec(memory_space=pl.ANY)] * 5,
        out_specs=pl.BlockSpec(memory_space=pltpu.VMEM),
        scratch_shapes=[
            pltpu.VMEM((tokens, width), jnp.bfloat16),
            pltpu.VMEM((tokens // LANES, LANES), jnp.int32),
            pltpu.VMEM((1, docs), jnp.int32),
            pltpu.VMEM((1, docs), jnp.int32),
            pltpu.VMEM((1, width), f32),
            pltpu.VMEM((n_seq, per_owner, width), f32),
            pltpu.VMEM((n_seq - 1, per_owner, width), f32),
            pltpu.VMEM((per_owner, LANES), f32),
            pltpu.VMEM((n_hid - 1, per_owner, LANES), f32),
            dma((chunks,)),
            dma((4,)),
            dma(()),
            dma(()),
            dma(()),
            dma(()),
        ],
        compiler_params=pltpu.CompilerParams(collective_id=0, has_side_effects=True),
    )(
        hidden,
        seg_ids.reshape(tokens // LANES, LANES),
        lengths.reshape(1, docs),
        owner_slot.reshape(1, docs),
        pool_bias.reshape(1, width),
    )


def solution(mesh):
    placed = (P("seq", "hid"), P("seq"), P(), P(), P("hid"))
    return jax.shard_map(
        functools.partial(local, mesh.shape["seq"], mesh.shape["hid"]),
        mesh=mesh,
        in_specs=placed,
        out_specs=P("seq", "hid"),
        check_vma=False,
    )
```

```python
import functools

import jax
import jax.numpy as jnp
from jax import lax
from jax.experimental import pallas as pl
from jax.experimental.pallas import tpu as pltpu
from jax.sharding import PartitionSpec as P

MESH = pl.DeviceIdType.MESH
LANES = 128


def kernel(
    n_seq, n_hid, chunks, urgent, pad,
    hidden_hbm, seg_hbm, len_hbm, slot_hbm, bias_hbm,
    out_ref,
    hidden, seg, lens, slots, bias, parts, landed, squares, squares_in,
    load_sems, small_sems, send_sem, recv_sem, sq_send_sem, sq_recv_sem,
):
    me = lax.axis_index("seq")
    my_hid = lax.axis_index("hid")
    tokens, width = hidden.shape
    docs = lens.shape[1]
    per_owner = docs // n_seq
    step = width // chunks
    features = width * n_hid
    peers = [jnp.where(j < me, j, j + 1) for j in range(n_seq - 1)]
    slot_there = [jnp.where(j < me, me - 1, me) for j in range(n_seq - 1)]
    hid_peers = {k: lax.rem(my_hid + k, n_hid) for k in range(1, n_hid)}

    def loader(c):
        cols = pl.ds(c * step, step)
        return pltpu.make_async_copy(hidden_hbm.at[:, cols], hidden.at[:, cols], load_sems.at[c])

    small = [
        pltpu.make_async_copy(src, dst, small_sems.at[i])
        for i, (src, dst) in enumerate(
            ((slot_hbm, slots), (seg_hbm, seg), (len_hbm, lens), (bias_hbm, bias))
        )
    ]
    small[0].start()
    small[1].start()
    loads = [loader(c) for c in range(chunks)]
    for load in loads:
        load.start()
    small[2].start()
    small[3].start()

    barrier = pltpu.get_barrier_semaphore()
    for peer in peers:
        pl.semaphore_signal(barrier, inc=1, device_id={"seq": peer}, device_id_type=MESH)
    for k in range(1, n_hid):
        pl.semaphore_signal(barrier, inc=1, device_id={"hid": hid_peers[k]}, device_id_type=MESH)

    small[0].wait()
    row = lax.broadcasted_iota(jnp.int32, (n_seq * pad, 1), 0)
    inner = row % pad
    row_slot = jnp.where(inner < per_owner, (row // pad) * per_owner + inner, -1)
    doc_iota = lax.broadcasted_iota(jnp.int32, (1, docs), 1).astype(jnp.float32)
    found = jnp.where(row_slot == slots[...], doc_iota + 1.0, 0.0)
    row_doc = jnp.sum(found, axis=1, keepdims=True).astype(jnp.int32) - 1
    small[1].wait()
    picker = jnp.concatenate(
        [
            jnp.where(row_doc == seg[k : k + 1, :], 1.0, 0.0).astype(jnp.bfloat16)
            for k in range(tokens // LANES)
        ],
        axis=1,
    )

    def send(cols, j):
        pltpu.make_async_remote_copy(
            src_ref=parts.at[peers[j], :, cols],
            dst_ref=landed.at[slot_there[j], :, cols],
            send_sem=send_sem,
            recv_sem=recv_sem,
            device_id={"seq": peers[j]},
            device_id_type=MESH,
        ).start()

    for c in range(chunks):
        cols = pl.ds(c * step, step)
        loads[c].wait()
        product = jnp.dot(picker, hidden[:, cols], preferred_element_type=jnp.float32)
        for p in range(n_seq):
            parts[p, :, cols] = product[p * pad : p * pad + per_owner, :]
        if c == 0:
            pl.semaphore_wait(barrier, n_seq - 1 + n_hid - 1)
        for j in range(urgent):
            send(cols, j)
    for j in range(urgent, n_seq - 1):
        send(pl.ds(0, width), j)

    small[2].wait()
    small[3].wait()
    wanted = lax.broadcasted_iota(jnp.int32, (per_owner, 1), 0) + me * per_owner
    my_len = jnp.sum(
        jnp.where(wanted == slots[...], lens[...].astype(jnp.float32), 0.0), axis=1, keepdims=True
    )

    pltpu.make_async_copy(landed, landed, recv_sem).wait()
    total = parts[me]
    for k in range(n_seq - 1):
        total = total + landed[k]
    averages = total / my_len + bias[...]
    lane_sq = jnp.zeros((per_owner, LANES), jnp.float32)
    for j in range(width // LANES):
        piece = averages[:, j * LANES : (j + 1) * LANES]
        lane_sq = lane_sq + piece * piece
    squares[...] = lane_sq

    for k in range(1, n_hid):
        pltpu.make_async_remote_copy(
            src_ref=squares,
            dst_ref=squares_in.at[k - 1],
            send_sem=sq_send_sem,
            recv_sem=sq_recv_sem,
            device_id={"hid": hid_peers[k]},
            device_id_type=MESH,
        ).start()
    pltpu.make_async_copy(landed, landed, send_sem).wait()
    pltpu.make_async_copy(squares_in, squares_in, sq_recv_sem).wait()
    for k in range(n_hid - 1):
        lane_sq = lane_sq + squares_in[k]
    energy = jnp.sum(lane_sq, axis=1, keepdims=True) / features
    out_ref[...] = (averages * lax.rsqrt(energy + 1e-06)).astype(jnp.bfloat16)
    pltpu.make_async_copy(squares_in, squares_in, sq_send_sem).wait()


def local(n_seq, n_hid, hidden, seg_ids, lengths, owner_slot, pool_bias):
    tokens, width = hidden.shape
    docs = lengths.shape[0]
    per_owner = docs // n_seq
    pad = -(-per_owner // 8) * 8
    chunks = 2
    urgent = max(1, n_seq // 4)
    f32 = jnp.float32
    dma = pltpu.SemaphoreType.DMA
    return pl.pallas_call(
        functools.partial(kernel, n_seq, n_hid, chunks, urgent, pad),
        out_shape=pltpu.VMEM((per_owner, width), jnp.bfloat16),
        in_specs=[pl.BlockSpec(memory_space=pl.ANY)] * 5,
        out_specs=pl.BlockSpec(memory_space=pltpu.VMEM),
        scratch_shapes=[
            pltpu.VMEM((tokens, width), jnp.bfloat16),
            pltpu.VMEM((tokens // LANES, LANES), jnp.int32),
            pltpu.VMEM((1, docs), jnp.int32),
            pltpu.VMEM((1, docs), jnp.int32),
            pltpu.VMEM((1, width), f32),
            pltpu.VMEM((n_seq, per_owner, width), f32),
            pltpu.VMEM((n_seq - 1, per_owner, width), f32),
            pltpu.VMEM((per_owner, LANES), f32),
            pltpu.VMEM((n_hid - 1, per_owner, LANES), f32),
            dma((chunks,)),
            dma((4,)),
            dma(()),
            dma(()),
            dma(()),
            dma(()),
        ],
        compiler_params=pltpu.CompilerParams(collective_id=0, has_side_effects=True),
    )(
        hidden,
        seg_ids.reshape(tokens // LANES, LANES),
        lengths.reshape(1, docs),
        owner_slot.reshape(1, docs),
        pool_bias.reshape(1, width),
    )


def solution(mesh):
    placed = (P("seq", "hid"), P("seq"), P(), P(), P("hid"))
    return jax.shard_map(
        functools.partial(local, mesh.shape["seq"], mesh.shape["hid"]),
        mesh=mesh,
        in_specs=placed,
        out_specs=P("seq", "hid"),
        check_vma=False,
    )
```

```python
import functools

import jax
import jax.numpy as jnp
from jax import lax
from jax.experimental import pallas as pl
from jax.experimental.pallas import tpu as pltpu
from jax.sharding import PartitionSpec as P

MESH = pl.DeviceIdType.MESH
LANES = 128


def kernel(
    n_seq, n_hid, chunks, urgent, pad,
    hidden_hbm, seg_hbm, len_hbm, slot_hbm, bias_hbm,
    out_ref,
    hidden, seg, lens, slots, bias, parts, landed, squares, squares_in,
    load_sems, small_sems, send_sem, recv_sem, sq_send_sem, sq_recv_sem,
):
    me = lax.axis_index("seq")
    my_hid = lax.axis_index("hid")
    tokens, width = hidden.shape
    docs = lens.shape[1]
    per_owner = docs // n_seq
    step = width // chunks
    features = width * n_hid
    peers = [jnp.where(j < me, j, j + 1) for j in range(n_seq - 1)]
    slot_there = [jnp.where(j < me, me - 1, me) for j in range(n_seq - 1)]
    hid_peers = {k: lax.rem(my_hid + k, n_hid) for k in range(1, n_hid)}

    def loader(c):
        cols = pl.ds(c * step, step)
        return pltpu.make_async_copy(hidden_hbm.at[:, cols], hidden.at[:, cols], load_sems.at[c])

    small = [
        pltpu.make_async_copy(src, dst, small_sems.at[i])
        for i, (src, dst) in enumerate(
            ((slot_hbm, slots), (seg_hbm, seg), (len_hbm, lens), (bias_hbm, bias))
        )
    ]
    small[0].start()
    small[1].start()
    loads = [loader(c) for c in range(chunks)]
    pieces = 4
    rows = tokens // pieces
    for c in range(chunks):
        cols = pl.ds(c * step, step)
        for r in range(pieces):
            part = pl.ds(r * rows, rows)
            pltpu.make_async_copy(
                hidden_hbm.at[part, cols], hidden.at[part, cols], load_sems.at[c]
            ).start()
    small[2].start()
    small[3].start()

    barrier = pltpu.get_barrier_semaphore()
    for peer in peers:
        pl.semaphore_signal(barrier, inc=1, device_id={"seq": peer}, device_id_type=MESH)
    for k in range(1, n_hid):
        pl.semaphore_signal(barrier, inc=1, device_id={"hid": hid_peers[k]}, device_id_type=MESH)

    small[0].wait()
    row = lax.broadcasted_iota(jnp.int32, (n_seq * pad, 1), 0)
    inner = row % pad
    row_slot = jnp.where(inner < per_owner, (row // pad) * per_owner + inner, -1)
    doc_iota = lax.broadcasted_iota(jnp.int32, (1, docs), 1).astype(jnp.float32)
    found = jnp.where(row_slot == slots[...], doc_iota + 1.0, 0.0)
    row_doc = jnp.sum(found, axis=1, keepdims=True).astype(jnp.int32) - 1
    small[1].wait()
    picker = jnp.concatenate(
        [
            jnp.where(row_doc == seg[k : k + 1, :], 1.0, 0.0).astype(jnp.bfloat16)
            for k in range(tokens // LANES)
        ],
        axis=1,
    )

    def send(cols, j):
        pltpu.make_async_remote_copy(
            src_ref=parts.at[peers[j], :, cols],
            dst_ref=landed.at[slot_there[j], :, cols],
            send_sem=send_sem,
            recv_sem=recv_sem,
            device_id={"seq": peers[j]},
            device_id_type=MESH,
        ).start()

    for c in range(chunks):
        cols = pl.ds(c * step, step)
        loads[c].wait()
        product = jnp.dot(picker, hidden[:, cols], preferred_element_type=jnp.float32)
        for p in range(n_seq):
            parts[p, :, cols] = product[p * pad : p * pad + per_owner, :]
        if c == 0:
            pl.semaphore_wait(barrier, n_seq - 1 + n_hid - 1)
        for j in range(urgent):
            send(cols, j)
    for j in range(urgent, n_seq - 1):
        send(pl.ds(0, width), j)

    small[2].wait()
    small[3].wait()
    wanted = lax.broadcasted_iota(jnp.int32, (per_owner, 1), 0) + me * per_owner
    my_len = jnp.sum(
        jnp.where(wanted == slots[...], lens[...].astype(jnp.float32), 0.0), axis=1, keepdims=True
    )

    pltpu.make_async_copy(landed, landed, recv_sem).wait()
    total = parts[me]
    for k in range(n_seq - 1):
        total = total + landed[k]
    averages = total / my_len + bias[...]
    lane_sq = jnp.zeros((per_owner, LANES), jnp.float32)
    for j in range(width // LANES):
        piece = averages[:, j * LANES : (j + 1) * LANES]
        lane_sq = lane_sq + piece * piece
    squares[...] = lane_sq

    for k in range(1, n_hid):
        pltpu.make_async_remote_copy(
            src_ref=squares,
            dst_ref=squares_in.at[k - 1],
            send_sem=sq_send_sem,
            recv_sem=sq_recv_sem,
            device_id={"hid": hid_peers[k]},
            device_id_type=MESH,
        ).start()
    pltpu.make_async_copy(landed, landed, send_sem).wait()
    pltpu.make_async_copy(squares_in, squares_in, sq_recv_sem).wait()
    for k in range(n_hid - 1):
        lane_sq = lane_sq + squares_in[k]
    energy = jnp.sum(lane_sq, axis=1, keepdims=True) / features
    out_ref[...] = (averages * lax.rsqrt(energy + 1e-06)).astype(jnp.bfloat16)
    pltpu.make_async_copy(squares_in, squares_in, sq_send_sem).wait()


def local(n_seq, n_hid, hidden, seg_ids, lengths, owner_slot, pool_bias):
    tokens, width = hidden.shape
    docs = lengths.shape[0]
    per_owner = docs // n_seq
    pad = -(-per_owner // 8) * 8
    chunks = 2
    urgent = max(1, n_seq // 4)
    f32 = jnp.float32
    dma = pltpu.SemaphoreType.DMA
    return pl.pallas_call(
        functools.partial(kernel, n_seq, n_hid, chunks, urgent, pad),
        out_shape=pltpu.VMEM((per_owner, width), jnp.bfloat16),
        in_specs=[pl.BlockSpec(memory_space=pl.ANY)] * 5,
        out_specs=pl.BlockSpec(memory_space=pltpu.VMEM),
        scratch_shapes=[
            pltpu.VMEM((tokens, width), jnp.bfloat16),
            pltpu.VMEM((tokens // LANES, LANES), jnp.int32),
            pltpu.VMEM((1, docs), jnp.int32),
            pltpu.VMEM((1, docs), jnp.int32),
            pltpu.VMEM((1, width), f32),
            pltpu.VMEM((n_seq, per_owner, width), f32),
            pltpu.VMEM((n_seq - 1, per_owner, width), f32),
            pltpu.VMEM((per_owner, LANES), f32),
            pltpu.VMEM((n_hid - 1, per_owner, LANES), f32),
            dma((chunks,)),
            dma((4,)),
            dma(()),
            dma(()),
            dma(()),
            dma(()),
        ],
        compiler_params=pltpu.CompilerParams(collective_id=0, has_side_effects=True),
    )(
        hidden,
        seg_ids.reshape(tokens // LANES, LANES),
        lengths.reshape(1, docs),
        owner_slot.reshape(1, docs),
        pool_bias.reshape(1, width),
    )


def solution(mesh):
    placed = (P("seq", "hid"), P("seq"), P(), P(), P("hid"))
    return jax.shard_map(
        functools.partial(local, mesh.shape["seq"], mesh.shape["hid"]),
        mesh=mesh,
        in_specs=placed,
        out_specs=P("seq", "hid"),
        check_vma=False,
    )
```
